32 devices in a mesh: dp: 32 (over z, y, x, core).
Axes of the slice: x: 2, y: 2, z: 4, core: 2. Of those that a mesh axis runs over, the one named last changes fastest.
Arguments:
- attended: bfloat16 [16384, 1152], P('dp'), may hold values from -24 to 24, as said below
- proj_cot: bfloat16 [16384, 1152], P('dp'), may hold values from -0.0007324219 to 0.0007324219
- timesteps: float32 [64], P('dp'), may hold values from 0 to 1
- embed_cot: bfloat16 [64, 1152], P('dp'), may hold values from -0.03125 to 0.03125
- master_proj: float32 [1327104], P('dp'), may hold values from -0.1875 to 0.1875
- moment_proj: float32 [1327104], P('dp'), may hold values from -0.013671875 to 0.013671875
- second_proj: float32 [1327104], P('dp'), may hold values from 1.8838011e-07 to 3.0140818e-06
- master_embed: float32 [294912], P('dp'), may hold values from -0.375 to 0.375
- moment_embed: float32 [294912], P('dp'), may hold values from -0.02734375 to 0.02734375
- squared_moment_layer: float32 [294912], P('dp'), may hold values from 8.477105e-07 to 1.3563368e-05
- attended_next: bfloat16 [16384, 1152], P('dp'), may hold values from -6 to 6
- timesteps_next: float32 [64], P('dp'), may hold values from 0 to 1
Outputs:
- next_proj: bfloat16 [16384, 1152], P('dp')
- next_embed: bfloat16 [64, 1152], P('dp')
- move_direction_output: float32 [1327104], P('dp')
- step_embed: float32 [294912], P('dp')
- master_proj_new: float32 [1327104], P('dp')
- master_embed_new: float32 [294912], P('dp')
- grad_norm: float32 [], replicated
The draws below stay inside these ranges and needn't reach their ends.
Inputs may be any that keep to these rules, and one draw needn't show every extreme that they name: attended has entries of mean zero whose scale differs between feature columns by up to a factor of 16.
All inputs are finite; a program needn't handle non-finite values.
Results may differ from the reference program's by a relative error of at most 0.0025.
Values may be sent and summed in bfloat16 or wider, within the bound.
A program may use at most 64 MiB of HBM per device.

```python
import math
import jax
import jax.numpy as jnp

MODEL_BREADTH = 1152
WAVE_EMBED_SPAN = 256
IMG_DEV = 2
TOK_DEV = 512
TOKENS = 16384
IMAGES = 64
N_DP = 32


def draw_attended(key, part):
    scale_key = jax.random.fold_in(key, 11)
    value_key = jax.random.fold_in(key, 12)
    log_scale = jax.random.uniform(scale_key, (MODEL_BREADTH,), jnp.float32, math.log(0.25), math.log(4.0))
    column_scale = jnp.exp(log_scale)
    values = jax.random.truncated_normal(value_key, -6.0, 6.0, (TOKENS, MODEL_BREADTH), jnp.float32)
    return (values * column_scale[None, :]).astype(jnp.bfloat16)


def level_of(rng, shape, shards, smallest, high):
    factor_of, own = 1.0, jax.random.fold_in(rng, 6)
    for dim, blocks in shards:
        heights = jnp.exp(jax.random.uniform(jax.random.fold_in(own, dim), (blocks,), jnp.float32, smallest / len(shards), high / len(shards)))
        factor_of = factor_of * jnp.repeat(heights, shape[dim] // blocks).reshape([-1 if axis == dim else 1 for axis in range(len(shape))])
    return factor_of


def centred(rng, dims, scale, reach, split=(), kind=jnp.bfloat16):
    level = level_of(rng, dims, split, -0.22, 0.18) if split else 1.0
    entries = jax.random.normal(rng, dims, jnp.float32) * scale * level
    return jnp.minimum(jnp.maximum(entries, -reach), reach).astype(kind)


def setup_inputs(seed: int = 0) -> dict:
    seeds = jax.random.split(jax.random.key(seed), 13)
    attended = draw_attended(jax.random.fold_in(seeds[12], 71), 0)
    proj_cot = centred(seeds[1], (TOKENS, MODEL_BREADTH), (7.0 / (MODEL_BREADTH * (TOK_DEV * N_DP) ** 0.5)), 0.0007324219, ((0, 32),))
    timesteps = jnp.clip(1.0 * jax.random.uniform(seeds[2], (IMAGES,), jnp.float32) ** level_of(seeds[2], (IMAGES,), ((0, 32),), -0.2, 0.2), 0.0, 1.0)
    embed_cot = centred(seeds[3], (IMAGES, MODEL_BREADTH), (10.0 / (WAVE_EMBED_SPAN * MODEL_BREADTH * IMG_DEV * N_DP) ** 0.5), 0.03125, ((0, 32),))
    master_proj = centred(seeds[4], (MODEL_BREADTH * MODEL_BREADTH,), MODEL_BREADTH ** -0.5, 0.1875, ((0, 32),), jnp.float32)
    moment_proj = centred(seeds[5], (MODEL_BREADTH * MODEL_BREADTH,), (1.0 / MODEL_BREADTH), 0.013671875, ((0, 32),), jnp.float32)
    second_proj = jnp.clip(jnp.exp(math.log(3.014081812580116e-06) - 2.7725887 * jax.random.uniform(seeds[6], (MODEL_BREADTH * MODEL_BREADTH,), jnp.float32) ** level_of(seeds[6], (MODEL_BREADTH * MODEL_BREADTH,), ((0, 32),), -0.2, 0.2)), 1.8838011328625726e-07, 3.014081812580116e-06)
    master_embed = centred(seeds[7], (WAVE_EMBED_SPAN * MODEL_BREADTH,), WAVE_EMBED_SPAN ** -0.5, 0.375, ((0, 32),), jnp.float32)
    moment_embed = centred(seeds[8], (WAVE_EMBED_SPAN * MODEL_BREADTH,), (1.0 / (WAVE_EMBED_SPAN * MODEL_BREADTH) ** 0.5), 0.02734375, ((0, 32),), jnp.float32)
    squared_moment_layer = jnp.clip(jnp.exp(math.log(1.3563368156610522e-05) - 2.7725887 * jax.random.uniform(seeds[9], (WAVE_EMBED_SPAN * MODEL_BREADTH,), jnp.float32) ** level_of(seeds[9], (WAVE_EMBED_SPAN * MODEL_BREADTH,), ((0, 32),), -0.2, 0.2)), 8.477105097881577e-07, 1.3563368156610522e-05)
    attended_next = centred(seeds[10], (TOKENS, MODEL_BREADTH), 1.0, 6.0, ((0, 32),))
    timesteps_next = jnp.clip(1.0 * jax.random.uniform(seeds[11], (IMAGES,), jnp.float32) ** level_of(seeds[11], (IMAGES,), ((0, 32),), -0.2, 0.2), 0.0, 1.0)
    return dict(attended=attended, proj_cot=proj_cot, timesteps=timesteps, embed_cot=embed_cot, master_proj=master_proj, moment_proj=moment_proj, second_proj=second_proj, master_embed=master_embed, moment_embed=moment_embed, squared_moment_layer=squared_moment_layer, attended_next=attended_next, timesteps_next=timesteps_next)


beta_one = 0.9
beta_two = 0.999
step_count = 1000.0
learn_rate = 0.0001
shrink_factor = 0.01
epsilon = 1e-08
max_norm = 1.0

def freq_embed(moments):
    half_width = WAVE_EMBED_SPAN // 2
    ladder = jnp.arange(half_width, dtype=jnp.float32)
    freqs = jnp.exp(-math.log(10000.0) * ladder / half_width)
    phase_values = (moments * 1000.0)[:, None] * freqs[None, :]
    return jnp.concatenate([jnp.cos(phase_values), jnp.sin(phase_values)], axis=1).astype(jnp.bfloat16)

def adamw_update(gradient, clip, master, moment, second):
    scaled = clip * gradient
    first_new = beta_one * moment + (1.0 - beta_one) * scaled
    second_new = beta_two * second + (1.0 - beta_two) * scaled * scaled
    first_hat = first_new / (1.0 - beta_one ** step_count)
    second_hat = second_new / (1.0 - beta_two ** step_count)
    direction = first_hat / (jnp.sqrt(second_hat) + epsilon)
    freshened_values = master - learn_rate * (direction + shrink_factor * master)
    return (direction, freshened_values)

def reference(attended, proj_cot, timesteps, embed_cot, master_proj, moment_proj, second_proj, master_embed, moment_embed, squared_moment_layer, attended_next, timesteps_next):
    grad_proj = jnp.dot(attended.T, proj_cot, preferred_element_type=jnp.float32).reshape(-1)
    freq_now = freq_embed(timesteps)
    grad_embed = jnp.dot(freq_now.T, embed_cot, preferred_element_type=jnp.float32).reshape(-1)
    total = jnp.sum(grad_proj * grad_proj) + jnp.sum(grad_embed * grad_embed)
    grad_norm = jnp.sqrt(total)
    clip = jnp.minimum(jnp.float32(1.0), max_norm / (grad_norm + 1e-06))
    move_direction_output, master_proj_new = adamw_update(grad_proj, clip, master_proj, moment_proj, second_proj)
    step_embed, master_embed_new = adamw_update(grad_embed, clip, master_embed, moment_embed, squared_moment_layer)
    weight_proj = master_proj_new.astype(jnp.bfloat16).reshape(MODEL_BREADTH, MODEL_BREADTH)
    weight_embed = master_embed_new.astype(jnp.bfloat16).reshape(WAVE_EMBED_SPAN, MODEL_BREADTH)
    next_proj = jnp.dot(attended_next, weight_proj, preferred_element_type=jnp.float32).astype(jnp.bfloat16)
    next_embed = jnp.dot(freq_embed(timesteps_next), weight_embed, preferred_element_type=jnp.float32).astype(jnp.bfloat16)
    return (next_proj, next_embed, move_direction_output, step_embed, master_proj_new, master_embed_new, grad_norm)
```

```python
import functools
import math

import jax
import jax.numpy as jnp
from jax import lax
from jax.experimental import pallas as pl
from jax.experimental.pallas import tpu as pltpu
from jax.sharding import PartitionSpec as P

beta_one = 0.9
beta_two = 0.999
step_count = 1000.0
learn_rate = 0.0001
shrink_factor = 0.01
epsilon = 1e-08
max_norm = 1.0


def freq_embed(moments, width):
    half_width = width // 2
    ladder = jnp.arange(half_width, dtype=jnp.float32)
    freqs = jnp.exp(-math.log(10000.0) * ladder / half_width)
    phase_values = (moments * 1000.0)[:, None] * freqs[None, :]
    return jnp.concatenate([jnp.cos(phase_values), jnp.sin(phase_values)], axis=1).astype(
        jnp.bfloat16
    )


def adamw_update(gradient, clip, master, moment, second):
    scaled = clip * gradient
    first_new = beta_one * moment + (1.0 - beta_one) * scaled
    second_new = beta_two * second + (1.0 - beta_two) * scaled * scaled
    first_hat = first_new / (1.0 - beta_one**step_count)
    second_hat = second_new / (1.0 - beta_two**step_count)
    direction = first_hat / (jnp.sqrt(second_hat) + epsilon)
    freshened_values = master - learn_rate * (direction + shrink_factor * master)
    return (direction, freshened_values)


LANES = 128
MESH = pl.DeviceIdType.MESH


def round_up(value, step):
    return -(-value // step) * step


def factor(n):
    bits = (n // 2).bit_length() - 1
    z_bits = -(-bits // 3)
    y_bits = -(-(bits - z_bits) // 2)
    return 2**z_bits, 2**y_bits, 2 ** (bits - z_bits - y_bits)


def exchange_kernel(
    n,
    rows,
    rows_embed,
    grad_p,
    grad_e,
    master_p,
    moment_p,
    second_p,
    master_e,
    moment_e,
    second_e,
    weight_p,
    weight_e,
    step_p,
    step_e,
    new_p,
    new_e,
    norm_out,
    stage,
    mine,
    g,
    r0,
    a1,
    r_a,
    a2,
    r_b,
    a3,
    r_z,
    norm_src,
    norm_all,
    w,
    c_sem,
    a_sem,
    b_sem,
    z_sem,
    n_sem,
    gz_sem,
    gb_sem,
    ga_sem,
    gc_sem,
):
    nz, ny, nx = factor(n)
    q = nx
    columns = grad_p.shape[1] // LANES
    flat_e = rows_embed * columns
    flat_p = rows * columns
    base_p = round_up(flat_e, 8)
    depth = g.shape[-2]
    group = stage.shape[0] // depth

    me = lax.axis_index("dp")
    c = lax.rem(me, 2)
    x = lax.rem(me // 2, nx)
    y = lax.rem(me // (2 * nx), ny)
    z = me // (2 * nx * ny)
    first = c == 0
    a, b = jnp.where(first, x, y), jnp.where(first, y, x)
    stride_a, stride_b = jnp.where(first, 2, 2 * nx), jnp.where(first, 2 * nx, 2)

    def device(z_at, a_at, b_at):
        return z_at * (2 * nx * ny) + a_at * stride_a + b_at * stride_b + c

    partner = me + 1 - 2 * c

    def place(d):
        core = lax.rem(d, 2)
        dx = lax.rem(d // 2, nx)
        dy = lax.rem(d // (2 * nx), ny)
        return (
            core,
            d // (2 * nx * ny),
            jnp.where(core == 0, dx, dy),
            jnp.where(core == 0, dy, dx),
        )

    def remote(src, dst, sems, at, target):
        return pltpu.make_async_remote_copy(
            src_ref=src,
            dst_ref=dst,
            send_sem=sems.at[(0, *at)],
            recv_sem=sems.at[(1, *at)],
            device_id=(target,),
            device_id_type=MESH,
        )

    barrier = pltpu.get_barrier_semaphore()

    @pl.loop(1, n)
    def _(r):
        pl.semaphore_signal(
            barrier, inc=1, device_id=(lax.rem(me + r, n),), device_id_type=MESH
        )

    stage[...] = jnp.zeros_like(stage)

    @pl.loop(0, n // group)
    def _(p):
        top_p = pl.multiple_of(p * (group * rows), 16)
        top_e = pl.multiple_of(p * (group * rows_embed), 16)
        for j in range(columns):
            lanes = slice(j * LANES, (j + 1) * LANES)
            values_p = grad_p[pl.ds(top_p, group * rows), lanes]
            values_e = grad_e[pl.ds(top_e, group * rows_embed), lanes]
            for i in range(group):
                stage[pl.ds(i * depth + base_p + j, rows, stride=columns), :] = values_p[
                    i * rows : (i + 1) * rows
                ]
                stage[pl.ds(i * depth + j, rows_embed, stride=columns), :] = values_e[
                    i * rows_embed : (i + 1) * rows_embed
                ]
        for i in range(group):
            core, dz, da, db = place(p * group + i)
            g[core, dz, da, db] = stage[i * depth : (i + 1) * depth].astype(g.dtype)

    pl.semaphore_wait(barrier, n - 1)

    order = [lax.rem(z + 1 + k, nz) for k in range(nz)]
    c_copies, a_copies, b_copies, z_copies = [], [], [], []
    for k, zk in enumerate(order):
        copy = remote(g.at[1 - c, zk], r0.at[zk], c_sem, (k,), partner)
        copy.start()
        c_copies.append(copy)
    for k, zk in enumerate(order):
        c_copies[k].wait_recv()
        for i in range(q):
            for j in range(q):
                a1[zk, i, j] = (
                    g[c, zk, i, j].astype(jnp.float32) + r0[zk, i, j].astype(jnp.float32)
                ).astype(a1.dtype)
        for s in range(1, q):
            to = lax.rem(a + s, q)
            copy = remote(
                a1.at[zk, to], r_a.at[s - 1, zk], a_sem, (s - 1, k), device(z, to, b)
            )
            copy.start()
            a_copies.append(copy)
    for k, zk in enumerate(order):
        for s in range(1, q):
            a_copies[k * (q - 1) + s - 1].wait_recv()
        for j in range(q):
            total = a1[zk, a, j].astype(jnp.float32)
            for s in range(1, q):
                total = total + r_a[s - 1, zk, j].astype(jnp.float32)
            a2[zk, j] = total.astype(a2.dtype)
        for s in range(1, q):
            to = lax.rem(b + s, q)
            copy = remote(
                a2.at[zk, to], r_b.at[s - 1, zk], b_sem, (s - 1, k), device(z, a, to)
            )
            copy.start()
            b_copies.append(copy)
    for k, zk in enumerate(order):
        for s in range(1, q):
            b_copies[k * (q - 1) + s - 1].wait_recv()
        total = a2[zk, b].astype(jnp.float32)
        for s in range(1, q):
            total = total + r_b[s - 1, zk].astype(jnp.float32)
        if k < nz - 1:
            a3[k] = total.astype(a3.dtype)
            copy = remote(a3.at[k], r_z.at[k], z_sem, (k,), device(zk, a, b))
            copy.start()
            z_copies.append(copy)
        else:
            mine[...] = total
    for copy in z_copies:
        copy.wait_recv()
    total = mine[...]
    for k in range(nz - 1):
        total = total + r_z[k].astype(jnp.float32)
    mine[...] = total

    norm_src[...] = jnp.sum(total * total, axis=0, keepdims=True)
    norm_all[me] = norm_src[...]

    @pl.loop(1, n)
    def _(r):
        remote(norm_src, norm_all.at[me], n_sem, (), lax.rem(me + r, n)).start()

    others = norm_all.at[pl.ds(0, n - 1)]
    norm_copies = remote(others, others, n_sem, (), partner)
    norm_copies.wait_recv()
    norm = jnp.sqrt(jnp.sum(jnp.sum(norm_all[...], axis=0), axis=1, keepdims=True))
    clip = jnp.minimum(jnp.float32(1.0), max_norm / (norm + 1e-06))
    norm_out[...] = jnp.broadcast_to(norm, norm_out.shape)

    step, new = adamw_update(
        mine[base_p : base_p + flat_p], clip, master_p[...], moment_p[...], second_p[...]
    )
    step_p[...] = step
    new_p[...] = new
    stage[base_p : base_p + flat_p] = new
    step, new = adamw_update(mine[:flat_e], clip, master_e[...], moment_e[...], second_e[...])
    step_e[...] = step
    new_e[...] = new
    stage[:flat_e] = new
    w[c, z, a, b] = stage[:depth].astype(w.dtype)

    sent = []

    def forward(block, z_at, sems, at, target):
        copy = remote(block, block, sems, at, target)
        copy.start()
        sent.append(copy)

    def back(index, by, size):
        return lax.rem(index + size - by, size)

    own = w.at[c, z, a, b]
    for k in range(nz - 1):
        forward(own, z, gz_sem, (k,), device(order[k], a, b))
    for t in range(nz):
        z_t = back(z, t, nz)
        block = w.at[c, z_t, a, b]
        if t:
            remote(block, block, gz_sem, (t - 1,), partner).wait_recv()
        for s in range(1, q):
            forward(block, z_t, ga_sem, (s - 1, t, 0), device(z, lax.rem(a + s, q), b))
        for s in range(1, q):
            forward(block, z_t, gb_sem, (s - 1, t), device(z, a, lax.rem(b + s, q)))
        forward(block, z_t, gc_sem, (t, 0, 0), partner)
    for t in range(nz):
        z_t = back(z, t, nz)
        for kb in range(1, q):
            block = w.at[c, z_t, a, back(b, kb, q)]
            remote(block, block, gb_sem, (kb - 1, t), partner).wait_recv()
            for s in range(1, q):
                forward(block, z_t, ga_sem, (s - 1, t, kb), device(z, lax.rem(a + s, q), b))
            forward(block, z_t, gc_sem, (t, kb, 0), partner)
    for t in range(nz):
        z_t = back(z, t, nz)
        for kb in range(q):
            for ka in range(1, q):
                block = w.at[c, z_t, back(a, ka, q), back(b, kb, q)]
                remote(block, block, ga_sem, (ka - 1, t, kb), partner).wait_recv()
                forward(block, z_t, gc_sem, (t, kb, ka), partner)
    for t in range(nz):
        for kb in range(q):
            for ka in range(q):
                block = w.at[1 - c, back(z, t, nz), back(b, ka, q), back(a, kb, q)]
                remote(block, block, gc_sem, (t, kb, ka), partner).wait_recv()

    @pl.loop(0, n // group)
    def _(p):
        top_p = pl.multiple_of(p * (group * rows), 16)
        top_e = pl.multiple_of(p * (group * rows_embed), 16)
        for i in range(group):
            core, dz, da, db = place(p * group + i)
            stage[i * depth : (i + 1) * depth] = w[core, dz, da, db].astype(jnp.float32)
        for j in range(columns):
            lanes = slice(j * LANES, (j + 1) * LANES)
            weight_p[pl.ds(top_p, group * rows), lanes] = jnp.concatenate(
                [
                    stage[pl.ds(i * depth + base_p + j, rows, stride=columns), :]
                    for i in range(group)
                ],
                axis=0,
            ).astype(weight_p.dtype)
            weight_e[pl.ds(top_e, group * rows_embed), lanes] = jnp.concatenate(
                [
                    stage[pl.ds(i * depth + j, rows_embed, stride=columns), :]
                    for i in range(group)
                ],
                axis=0,
            ).astype(weight_e.dtype)

    for copy in c_copies + a_copies + b_copies + z_copies + sent:
        copy.wait_send()
    norm_copies.wait_send()


def exchange(n, grad_p, grad_e, states):
    nz, ny, nx = factor(n)
    width = grad_p.shape[1]
    columns = width // LANES
    rows, rows_embed = grad_p.shape[0] // n, grad_e.shape[0] // n
    group = max(16 // math.gcd(rows, 16), 16 // math.gcd(rows_embed, 16))
    depth = round_up(round_up(rows_embed * columns, 8) + rows * columns, 16)
    f32, bf16 = jnp.float32, jnp.bfloat16
    q = nx
    assert nx == ny and n % group == 0

    def dma(*sizes):
        return pltpu.SemaphoreType.DMA((2, *(max(size, 1) for size in sizes)))

    flat_p = jax.ShapeDtypeStruct((rows * columns, LANES), f32)
    flat_e = jax.ShapeDtypeStruct((rows_embed * columns, LANES), f32)
    vmem = pl.BlockSpec(memory_space=pltpu.VMEM)
    return pl.pallas_call(
        functools.partial(exchange_kernel, n, rows, rows_embed),
        out_shape=(
            jax.ShapeDtypeStruct(grad_p.shape, bf16),
            jax.ShapeDtypeStruct(grad_e.shape, bf16),
            flat_p,
            flat_e,
            flat_p,
            flat_e,
            jax.ShapeDtypeStruct((1, LANES), f32),
        ),
        in_specs=[vmem] * 8,
        out_specs=(vmem,) * 7,
        scratch_shapes=[
            pltpu.VMEM((group * depth, LANES), f32),
            pltpu.VMEM((depth, LANES), f32),
            pltpu.VMEM((2, nz, q, q, depth, LANES), bf16),
            pltpu.VMEM((nz, q, q, depth, LANES), bf16),
            pltpu.VMEM((nz, q, q, depth, LANES), bf16),
            pltpu.VMEM((q - 1, nz, q, depth, LANES), bf16),
            pltpu.VMEM((nz, q, depth, LANES), bf16),
            pltpu.VMEM((q - 1, nz, depth, LANES), bf16),
            pltpu.VMEM((nz - 1, depth, LANES), bf16),
            pltpu.VMEM((nz - 1, depth, LANES), bf16),
            pltpu.VMEM((1, LANES), f32),
            pltpu.VMEM((n, 1, LANES), f32),
            pltpu.VMEM((2, nz, q, q, depth, LANES), bf16),
            dma(nz),
            dma(q - 1, nz),
            dma(q - 1, nz),
            dma(nz - 1),
            dma(),
            dma(nz - 1),
            dma(q - 1, nz),
            dma(q - 1, nz, q),
            dma(nz, q, q),
        ],
        compiler_params=pltpu.CompilerParams(
            collective_id=0, has_side_effects=True, vmem_limit_bytes=56 * 2**20
        ),
    )(grad_p, grad_e, *(state.reshape(-1, LANES) for state in states))


def per_device(
    attended,
    proj_cot,
    timesteps,
    embed_cot,
    master_proj,
    moment_proj,
    second_proj,
    master_embed,
    moment_embed,
    squared_moment_layer,
    attended_next,
    timesteps_next,
):
    width = attended.shape[1]
    freq_width = master_embed.shape[0] * lax.axis_size("dp") // width
    n = lax.axis_size("dp")
    grad_proj = jnp.dot(attended.T, proj_cot, preferred_element_type=jnp.float32)
    freq_now = freq_embed(timesteps, freq_width)
    grad_embed = jnp.dot(freq_now.T, embed_cot, preferred_element_type=jnp.float32)
    states = (
        master_proj,
        moment_proj,
        second_proj,
        master_embed,
        moment_embed,
        squared_moment_layer,
    )
    weight_proj, weight_embed, step_p, step_e, new_p, new_e, norm = exchange(
        n, grad_proj, grad_embed, states
    )
    next_proj = jnp.dot(attended_next, weight_proj, preferred_element_type=jnp.float32).astype(
        jnp.bfloat16
    )
    freq_next = freq_embed(timesteps_next, freq_width)
    next_embed = jnp.dot(freq_next, weight_embed, preferred_element_type=jnp.float32).astype(
        jnp.bfloat16
    )
    return (
        next_proj,
        next_embed,
        step_p.reshape(-1),
        step_e.reshape(-1),
        new_p.reshape(-1),
        new_e.reshape(-1),
        norm[0, 0],
    )


def solution(mesh):
    in_specs = (
        P("dp", None),
        P("dp", None),
        P("dp"),
        P("dp", None),
        P("dp"),
        P("dp"),
        P("dp"),
        P("dp"),
        P("dp"),
        P("dp"),
        P("dp", None),
        P("dp"),
    )
    out_specs = (P("dp", None), P("dp", None), P("dp"), P("dp"), P("dp"), P("dp"), P())
    return jax.shard_map(
        per_device, mesh=mesh, in_specs=in_specs, out_specs=out_specs, check_vma=False
    )
```

```python
import functools
import math

import jax
import jax.numpy as jnp
from jax import lax
from jax.experimental import pallas as pl
from jax.experimental.pallas import tpu as pltpu
from jax.sharding import PartitionSpec as P

beta_one = 0.9
beta_two = 0.999
step_count = 1000.0
learn_rate = 0.0001
shrink_factor = 0.01
epsilon = 1e-08
max_norm = 1.0


def freq_embed(moments, width):
    half_width = width // 2
    ladder = jnp.arange(half_width, dtype=jnp.float32)
    freqs = jnp.exp(-math.log(10000.0) * ladder / half_width)
    phase_values = (moments * 1000.0)[:, None] * freqs[None, :]
    return jnp.concatenate([jnp.cos(phase_values), jnp.sin(phase_values)], axis=1).astype(
        jnp.bfloat16
    )


def adamw_update(gradient, clip, master, moment, second):
    scaled = clip * gradient
    first_new = beta_one * moment + (1.0 - beta_one) * scaled
    second_new = beta_two * second + (1.0 - beta_two) * scaled * scaled
    first_hat = first_new / (1.0 - beta_one**step_count)
    second_hat = second_new / (1.0 - beta_two**step_count)
    direction = first_hat / (jnp.sqrt(second_hat) + epsilon)
    freshened_values = master - learn_rate * (direction + shrink_factor * master)
    return (direction, freshened_values)


LANES = 128
MESH = pl.DeviceIdType.MESH


def round_up(value, step):
    return -(-value // step) * step


def factor(n):
    bits = (n // 2).bit_length() - 1
    z_bits = -(-bits // 3)
    y_bits = -(-(bits - z_bits) // 2)
    return 2**z_bits, 2**y_bits, 2 ** (bits - z_bits - y_bits)


def exchange_kernel(
    n,
    rows,
    rows_embed,
    attended,
    proj_cot,
    freq_now,
    embed_cot,
    attended_next,
    freq_next,
    master_p,
    moment_p,
    second_p,
    master_e,
    moment_e,
    second_e,
    next_p,
    next_e,
    step_p,
    step_e,
    new_p,
    new_e,
    norm_out,
    grad_p,
    grad_e,
    weight_p,
    weight_e,
    stage,
    mine,
    g,
    r0,
    a1,
    r_a,
    a2,
    r_b,
    a3,
    r_z,
    norm_src,
    norm_all,
    w,
    c_sem,
    a_sem,
    b_sem,
    z_sem,
    n_sem,
    gz_sem,
    gb_sem,
    ga_sem,
    gc_sem,
):
    nz, ny, nx = factor(n)
    q = nx
    columns = grad_p.shape[1] // LANES
    flat_e = rows_embed * columns
    flat_p = rows * columns
    base_p = round_up(flat_e, 8)
    depth = g.shape[-2]
    group = stage.shape[0] // depth

    me = lax.axis_index("dp")
    c = lax.rem(me, 2)
    x = lax.rem(me // 2, nx)
    y = lax.rem(me // (2 * nx), ny)
    z = me // (2 * nx * ny)
    first = c == 0
    a, b = jnp.where(first, x, y), jnp.where(first, y, x)
    stride_a, stride_b = jnp.where(first, 2, 2 * nx), jnp.where(first, 2 * nx, 2)

    def device(z_at, a_at, b_at):
        return z_at * (2 * nx * ny) + a_at * stride_a + b_at * stride_b + c

    partner = me + 1 - 2 * c

    def place(d):
        core = lax.rem(d, 2)
        dx = lax.rem(d // 2, nx)
        dy = lax.rem(d // (2 * nx), ny)
        return (
            core,
            d // (2 * nx * ny),
            jnp.where(core == 0, dx, dy),
            jnp.where(core == 0, dy, dx),
        )

    def remote(src, dst, sems, at, target):
        return pltpu.make_async_remote_copy(
            src_ref=src,
            dst_ref=dst,
            send_sem=sems.at[(0, *at)],
            recv_sem=sems.at[(1, *at)],
            device_id=(target,),
            device_id_type=MESH,
        )

    barrier = pltpu.get_barrier_semaphore()

    @pl.loop(1, n)
    def _(r):
        pl.semaphore_signal(
            barrier, inc=1, device_id=(lax.rem(me + r, n),), device_id_type=MESH
        )

    span = block_of(attended.shape[1])

    @pl.loop(0, attended.shape[1] // span)
    def _(i):
        top = pl.multiple_of(i * span, span)
        grad_p[pl.ds(top, span), :] = lax.dot_general(
            attended[:, pl.ds(top, span)],
            proj_cot[...],
            (((0,), (0,)), ((), ())),
            preferred_element_type=jnp.float32,
        )

    total = None
    for i in range(embed_cot.shape[0]):
        term = freq_now[:, i : i + 1] * embed_cot[i : i + 1, :].astype(jnp.float32)
        total = term if total is None else total + term
    grad_e[...] = total

    stage[...] = jnp.zeros_like(stage)
    order = [lax.rem(z + 1 + k, nz) for k in range(nz)]
    groups = n // group // nz
    c_copies, a_copies, b_copies, z_copies = [], [], [], []

    def flatten(zk):
        @pl.loop(zk * groups, zk * groups + groups)
        def _(p):
            top_p = pl.multiple_of(p * (group * rows), 16)
            top_e = pl.multiple_of(p * (group * rows_embed), 16)
            for j in range(columns):
                lanes = slice(j * LANES, (j + 1) * LANES)
                values_p = grad_p[pl.ds(top_p, group * rows), lanes]
                values_e = grad_e[pl.ds(top_e, group * rows_embed), lanes]
                for i in range(group):
                    stage[pl.ds(i * depth + base_p + j, rows, stride=columns), :] = values_p[
                        i * rows : (i + 1) * rows
                    ]
                    stage[pl.ds(i * depth + j, rows_embed, stride=columns), :] = values_e[
                        i * rows_embed : (i + 1) * rows_embed
                    ]
            for i in range(group):
                core, dz, da, db = place(p * group + i)
                g[core, dz, da, db] = stage[i * depth : (i + 1) * depth].astype(g.dtype)

    def reduce_core(k):
        zk = order[k]
        c_copies[k].wait_recv()
        for s in range(1, q + 1):
            i = lax.rem(a + s, q)
            for j in range(q):
                a1[zk, i, j] = (
                    g[c, zk, i, j].astype(jnp.float32) + r0[zk, i, j].astype(jnp.float32)
                ).astype(a1.dtype)
            if s < q:
                copy = remote(
                    a1.at[zk, i], r_a.at[s - 1, zk], a_sem, (s - 1, k), device(z, i, b)
                )
                copy.start()
                a_copies.append(copy)

    def reduce_a(k):
        zk = order[k]
        for s in range(1, q):
            a_copies[k * (q - 1) + s - 1].wait_recv()
        for s in range(1, q + 1):
            j = lax.rem(b + s, q)
            total = a1[zk, a, j].astype(jnp.float32)
            for r in range(1, q):
                total = total + r_a[r - 1, zk, j].astype(jnp.float32)
            a2[zk, j] = total.astype(a2.dtype)
            if s < q:
                copy = remote(
                    a2.at[zk, j], r_b.at[s - 1, zk], b_sem, (s - 1, k), device(z, a, j)
                )
                copy.start()
                b_copies.append(copy)

    def reduce_b(k):
        zk = order[k]
        for s in range(1, q):
            b_copies[k * (q - 1) + s - 1].wait_recv()
        total = a2[zk, b].astype(jnp.float32)
        for s in range(1, q):
            total = total + r_b[s - 1, zk].astype(jnp.float32)
        if k < nz - 1:
            a3[k] = total.astype(a3.dtype)
            copy = remote(a3.at[k], r_z.at[k], z_sem, (k,), device(zk, a, b))
            copy.start()
            z_copies.append(copy)
        else:
            mine[...] = total

    for k in range(nz + 3):
        if k < nz:
            flatten(order[k])
            if k == 0:
                pl.semaphore_wait(barrier, n - 1)
            copy = remote(g.at[1 - c, order[k]], r0.at[order[k]], c_sem, (k,), partner)
            copy.start()
            c_copies.append(copy)
        if 0 <= k - 1 < nz:
            reduce_core(k - 1)
        if 0 <= k - 2 < nz:
            reduce_a(k - 2)
        if 0 <= k - 3 < nz:
            reduce_b(k - 3)
    for copy in z_copies:
        copy.wait_recv()
    total = mine[...]
    for k in range(nz - 1):
        total = total + r_z[k].astype(jnp.float32)
    mine[...] = total

    norm_src[...] = jnp.sum(total * total, axis=0, keepdims=True)
    norm_all[me] = norm_src[...]

    @pl.loop(1, n)
    def _(r):
        remote(norm_src, norm_all.at[me], n_sem, (), lax.rem(me + r, n)).start()

    others = norm_all.at[pl.ds(0, n - 1)]
    norm_copies = remote(others, others, n_sem, (), partner)
    norm_copies.wait_recv()
    norm = jnp.sqrt(jnp.sum(jnp.sum(norm_all[...], axis=0), axis=1, keepdims=True))
    clip = jnp.minimum(jnp.float32(1.0), max_norm / (norm + 1e-06))
    norm_out[...] = jnp.broadcast_to(norm, norm_out.shape)

    step, new = adamw_update(
        mine[base_p : base_p + flat_p], clip, master_p[...], moment_p[...], second_p[...]
    )
    step_p[...] = step
    new_p[...] = new
    stage[base_p : base_p + flat_p] = new
    step, new = adamw_update(mine[:flat_e], clip, master_e[...], moment_e[...], second_e[...])
    step_e[...] = step
    new_e[...] = new
    stage[:flat_e] = new
    w[c, z, a, b] = stage[:depth].astype(w.dtype)

    sent = []

    def forward(block, z_at, sems, at, target):
        copy = remote(block, block, sems, at, target)
        copy.start()
        sent.append(copy)

    def back(index, by, size):
        return lax.rem(index + size - by, size)

    own = w.at[c, z, a, b]
    for k in range(nz - 1):
        forward(own, z, gz_sem, (k,), device(order[k], a, b))

    def gather_z(t):
        z_t = back(z, t, nz)
        block = w.at[c, z_t, a, b]
        if t:
            remote(block, block, gz_sem, (t - 1,), partner).wait_recv()
        for s in range(1, q):
            forward(block, z_t, gb_sem, (s - 1, t), device(z, a, lax.rem(b + s, q)))
        for s in range(1, q):
            forward(block, z_t, ga_sem, (s - 1, t, 0), device(z, lax.rem(a + s, q), b))
        forward(block, z_t, gc_sem, (t, 0, 0), partner)

    def gather_b(t):
        z_t = back(z, t, nz)
        for kb in range(1, q):
            block = w.at[c, z_t, a, back(b, kb, q)]
            remote(block, block, gb_sem, (kb - 1, t), partner).wait_recv()
            for s in range(1, q):
                forward(block, z_t, ga_sem, (s - 1, t, kb), device(z, lax.rem(a + s, q), b))
            forward(block, z_t, gc_sem, (t, kb, 0), partner)

    def gather_a(t):
        z_t = back(z, t, nz)
        for kb in range(q):
            for ka in range(1, q):
                block = w.at[c, z_t, back(a, ka, q), back(b, kb, q)]
                remote(block, block, ga_sem, (ka - 1, t, kb), partner).wait_recv()
                forward(block, z_t, gc_sem, (t, kb, ka), partner)

    def unflatten(t):
        z_t = back(z, t, nz)
        for kb in range(q):
            for ka in range(q):
                block = w.at[1 - c, z_t, back(b, ka, q), back(a, kb, q)]
                remote(block, block, gc_sem, (t, kb, ka), partner).wait_recv()

        @pl.loop(z_t * groups, z_t * groups + groups)
        def _(p):
            top_p = pl.multiple_of(p * (group * rows), 16)
            top_e = pl.multiple_of(p * (group * rows_embed), 16)
            for i in range(group):
                core, dz, da, db = place(p * group + i)
                stage[i * depth : (i + 1) * depth] = w[core, dz, da, db].astype(jnp.float32)
            for j in range(columns):
                lanes = slice(j * LANES, (j + 1) * LANES)
                weight_p[pl.ds(top_p, group * rows), lanes] = jnp.concatenate(
                    [
                        stage[pl.ds(i * depth + base_p + j, rows, stride=columns), :]
                        for i in range(group)
                    ],
                    axis=0,
                ).astype(weight_p.dtype)
                weight_e[pl.ds(top_e, group * rows_embed), lanes] = jnp.concatenate(
                    [
                        stage[pl.ds(i * depth + j, rows_embed, stride=columns), :]
                        for i in range(group)
                    ],
                    axis=0,
                ).astype(weight_e.dtype)

    for t in range(nz + 3):
        if t < nz:
            gather_z(t)
        if 0 <= t - 1 < nz:
            gather_b(t - 1)
        if 0 <= t - 2 < nz:
            gather_a(t - 2)
        if 0 <= t - 3 < nz:
            unflatten(t - 3)

    next_e[...] = jnp.dot(
        freq_next[...], weight_e[...], preferred_element_type=jnp.float32
    ).astype(next_e.dtype)

    @pl.loop(0, weight_p.shape[1] // span)
    def _(i):
        left = pl.multiple_of(i * span, span)
        next_p[:, pl.ds(left, span)] = jnp.dot(
            attended_next[...], weight_p[:, pl.ds(left, span)], preferred_element_type=jnp.float32
        ).astype(next_p.dtype)

    for copy in c_copies + a_copies + b_copies + z_copies + sent:
        copy.wait_send()
    norm_copies.wait_send()


def block_of(width):
    return next(size for size in (384, 256, 128) if width % size == 0)


def copy_kernel(*refs):
    half = len(refs) // 2
    for source, result in zip(refs[:half], refs[half:]):
        result[...] = source[...]


def exchange(n, attended, proj_cot, freq_now, embed_cot, attended_next, freq_next, states):
    nz, ny, nx = factor(n)
    width = attended.shape[1]
    width_e = freq_now.shape[0]
    columns = width // LANES
    rows, rows_embed = width // n, width_e // n
    group = max(16 // math.gcd(rows, 16), 16 // math.gcd(rows_embed, 16))
    depth = round_up(round_up(rows_embed * columns, 8) + rows * columns, 16)
    f32, bf16 = jnp.float32, jnp.bfloat16
    q = nx
    assert nx == ny and n % (group * nz) == 0

    def dma(*sizes):
        return pltpu.SemaphoreType.DMA((2, *(max(size, 1) for size in sizes)))

    flat_p = jax.ShapeDtypeStruct((rows * columns, LANES), f32)
    flat_e = jax.ShapeDtypeStruct((rows_embed * columns, LANES), f32)
    vmem = pl.BlockSpec(memory_space=pltpu.VMEM)
    results = (
        jax.ShapeDtypeStruct(attended_next.shape, bf16),
        jax.ShapeDtypeStruct(embed_cot.shape, bf16),
        flat_p,
        flat_e,
        flat_p,
        flat_e,
        jax.ShapeDtypeStruct((1, LANES), f32),
    )
    outs = pl.pallas_call(
        functools.partial(exchange_kernel, n, rows, rows_embed),
        out_shape=results,
        in_specs=[vmem] * 12,
        out_specs=(vmem,) * 7,
        scratch_shapes=[
            pltpu.VMEM((width, width), f32),
            pltpu.VMEM((width_e, width), f32),
            pltpu.VMEM((width, width), bf16),
            pltpu.VMEM((width_e, width), bf16),
            pltpu.VMEM((group * depth, LANES), f32),
            pltpu.VMEM((depth, LANES), f32),
            pltpu.VMEM((2, nz, q, q, depth, LANES), bf16),
            pltpu.VMEM((nz, q, q, depth, LANES), bf16),
            pltpu.VMEM((nz, q, q, depth, LANES), bf16),
            pltpu.VMEM((q - 1, nz, q, depth, LANES), bf16),
            pltpu.VMEM((nz, q, depth, LANES), bf16),
            pltpu.VMEM((q - 1, nz, depth, LANES), bf16),
            pltpu.VMEM((nz - 1, depth, LANES), bf16),
            pltpu.VMEM((nz - 1, depth, LANES), bf16),
            pltpu.VMEM((1, LANES), f32),
            pltpu.VMEM((n, 1, LANES), f32),
            pltpu.VMEM((2, nz, q, q, depth, LANES), bf16),
            dma(nz),
            dma(q - 1, nz),
            dma(q - 1, nz),
            dma(nz - 1),
            dma(),
            dma(nz - 1),
            dma(q - 1, nz),
            dma(q - 1, nz, q),
            dma(nz, q, q),
        ],
        compiler_params=pltpu.CompilerParams(
            collective_id=0, has_side_effects=True, vmem_limit_bytes=44 * 2**20
        ),
    )(
        attended,
        proj_cot,
        freq_now,
        embed_cot,
        attended_next,
        freq_next,
        *(state.reshape(-1, LANES) for state in states),
    )
    return pl.pallas_call(
        copy_kernel, out_shape=results, in_specs=[vmem] * 7, out_specs=(vmem,) * 7
    )(*outs)


def per_device(
    attended,
    proj_cot,
    timesteps,
    embed_cot,
    master_proj,
    moment_proj,
    second_proj,
    master_embed,
    moment_embed,
    squared_moment_layer,
    attended_next,
    timesteps_next,
):
    width = attended.shape[1]
    freq_width = master_embed.shape[0] * lax.axis_size("dp") // width
    n = lax.axis_size("dp")
    freq_now = freq_embed(timesteps, freq_width).astype(jnp.float32).T
    freq_next = freq_embed(timesteps_next, freq_width)
    states = (
        master_proj,
        moment_proj,
        second_proj,
        master_embed,
        moment_embed,
        squared_moment_layer,
    )
    next_proj, next_embed, step_p, step_e, new_p, new_e, norm = exchange(
        n, attended, proj_cot, freq_now, embed_cot, attended_next, freq_next, states
    )
    return (
        next_proj,
        next_embed,
        step_p.reshape(-1),
        step_e.reshape(-1),
        new_p.reshape(-1),
        new_e.reshape(-1),
        norm[0, 0],
    )


def solution(mesh):
    in_specs = (
        P("dp", None),
        P("dp", None),
        P("dp"),
        P("dp", None),
        P("dp"),
        P("dp"),
        P("dp"),
        P("dp"),
        P("dp"),
        P("dp"),
        P("dp", None),
        P("dp"),
    )
    out_specs = (P("dp", None), P("dp", None), P("dp"), P("dp"), P("dp"), P("dp"), P())
    return jax.shard_map(
        per_device, mesh=mesh, in_specs=in_specs, out_specs=out_specs, check_vma=False
    )
```

```python
import functools
import math

import jax
import jax.numpy as jnp
from jax import lax
from jax.experimental import pallas as pl
from jax.experimental.pallas import tpu as pltpu
from jax.sharding import PartitionSpec as P

beta_one = 0.9
beta_two = 0.999
step_count = 1000.0
learn_rate = 0.0001
shrink_factor = 0.01
epsilon = 1e-08
max_norm = 1.0


def freq_embed(moments, width):
    half_width = width // 2
    ladder = jnp.arange(half_width, dtype=jnp.float32)
    freqs = jnp.exp(-math.log(10000.0) * ladder / half_width)
    phase_values = (moments * 1000.0)[:, None] * freqs[None, :]
    return jnp.concatenate([jnp.cos(phase_values), jnp.sin(phase_values)], axis=1).astype(
        jnp.bfloat16
    )


def adamw_update(gradient, clip, master, moment, second):
    scaled = clip * gradient
    first_new = beta_one * moment + (1.0 - beta_one) * scaled
    second_new = beta_two * second + (1.0 - beta_two) * scaled * scaled
    first_hat = first_new / (1.0 - beta_one**step_count)
    second_hat = second_new / (1.0 - beta_two**step_count)
    direction = first_hat / (jnp.sqrt(second_hat) + epsilon)
    freshened_values = master - learn_rate * (direction + shrink_factor * master)
    return (direction, freshened_values)


LANES = 128
VMEM_LIMIT = 62 * 2**20
MESH = pl.DeviceIdType.MESH


def round_up(value, step):
    return -(-value // step) * step


def factor(n):
    bits = (n // 2).bit_length() - 1
    z_bits = -(-bits // 3)
    y_bits = -(-(bits - z_bits) // 2)
    return 2**z_bits, 2**y_bits, 2 ** (bits - z_bits - y_bits)


def exchange_kernel(
    n,
    rows,
    rows_embed,
    attended,
    proj_cot,
    freq_now,
    embed_cot,
    attended_next,
    freq_next,
    master_p,
    moment_p,
    second_p,
    master_e,
    moment_e,
    second_e,
    next_p,
    next_e,
    step_p,
    step_e,
    new_p,
    new_e,
    norm_out,
    grad_p,
    grad_e,
    weight_p,
    weight_e,
    stage,
    mine,
    g,
    r0,
    a1,
    r_a,
    a2,
    r_b,
    a3,
    r_z,
    norm_src,
    norm_all,
    w,
    c_sem,
    a_sem,
    b_sem,
    z_sem,
    n_sem,
    gz_sem,
    gb_sem,
    ga_sem,
    gc_sem,
):
    nz, ny, nx = factor(n)
    q = nx
    columns = grad_p.shape[1] // LANES
    flat_e = rows_embed * columns
    flat_p = rows * columns
    base_p = round_up(flat_e, 8)
    depth = g.shape[-2]
    group = stage.shape[0] // depth

    me = lax.axis_index("dp")
    c = lax.rem(me, 2)
    x = lax.rem(me // 2, nx)
    y = lax.rem(me // (2 * nx), ny)
    z = me // (2 * nx * ny)
    first = c == 0
    a, b = jnp.where(first, x, y), jnp.where(first, y, x)
    stride_a, stride_b = jnp.where(first, 2, 2 * nx), jnp.where(first, 2 * nx, 2)

    def device(z_at, a_at, b_at):
        return z_at * (2 * nx * ny) + a_at * stride_a + b_at * stride_b + c

    partner = me + 1 - 2 * c

    def place(d):
        core = lax.rem(d, 2)
        dx = lax.rem(d // 2, nx)
        dy = lax.rem(d // (2 * nx), ny)
        return (
            core,
            d // (2 * nx * ny),
            jnp.where(core == 0, dx, dy),
            jnp.where(core == 0, dy, dx),
        )

    def remote(src, dst, sems, at, target):
        return pltpu.make_async_remote_copy(
            src_ref=src,
            dst_ref=dst,
            send_sem=sems.at[(0, *at)],
            recv_sem=sems.at[(1, *at)],
            device_id=(target,),
            device_id_type=MESH,
        )

    barrier = pltpu.get_barrier_semaphore()

    @pl.loop(1, n)
    def _(r):
        pl.semaphore_signal(
            barrier, inc=1, device_id=(lax.rem(me + r, n),), device_id_type=MESH
        )

    span = block_of(attended.shape[1])

    @pl.loop(0, attended.shape[1] // span)
    def _(i):
        top = pl.multiple_of(i * span, span)
        grad_p[pl.ds(top, span), :] = lax.dot_general(
            attended[:, pl.ds(top, span)],
            proj_cot[...],
            (((0,), (0,)), ((), ())),
            preferred_element_type=jnp.float32,
        )

    total = None
    for i in range(embed_cot.shape[0]):
        term = freq_now[:, i : i + 1] * embed_cot[i : i + 1, :].astype(jnp.float32)
        total = term if total is None else total + term
    grad_e[...] = total

    stage[...] = jnp.zeros_like(stage)
    order = [lax.rem(z + 1 + k, nz) for k in range(nz)]
    groups = n // group // nz
    c_copies, a_copies, b_copies, z_copies = [], [], [], []

    def flatten(zk):
        @pl.loop(zk * groups, zk * groups + groups)
        def _(p):
            top_p = pl.multiple_of(p * (group * rows), 16)
            top_e = pl.multiple_of(p * (group * rows_embed), 16)
            for j in range(columns):
                lanes = slice(j * LANES, (j + 1) * LANES)
                values_p = grad_p[pl.ds(top_p, group * rows), lanes]
                values_e = grad_e[pl.ds(top_e, group * rows_embed), lanes]
                for i in range(group):
                    stage[pl.ds(i * depth + base_p + j, rows, stride=columns), :] = values_p[
                        i * rows : (i + 1) * rows
                    ]
                    stage[pl.ds(i * depth + j, rows_embed, stride=columns), :] = values_e[
                        i * rows_embed : (i + 1) * rows_embed
                    ]
            for i in range(group):
                core, dz, da, db = place(p * group + i)
                g[core, dz, da, db] = stage[i * depth : (i + 1) * depth].astype(g.dtype)

    def reduce_core(k):
        zk = order[k]
        c_copies[k].wait_recv()
        for s in range(1, q + 1):
            i = lax.rem(a + s, q)
            for j in range(q):
                a1[zk, i, j] = (
                    g[c, zk, i, j].astype(jnp.float32) + r0[zk, i, j].astype(jnp.float32)
                ).astype(a1.dtype)
            if s < q:
                copy = remote(
                    a1.at[zk, i], r_a.at[s - 1, zk], a_sem, (s - 1, k), device(z, i, b)
                )
                copy.start()
                a_copies.append(copy)

    def reduce_a(k):
        zk = order[k]
        for s in range(1, q):
            a_copies[k * (q - 1) + s - 1].wait_recv()
        for s in range(1, q + 1):
            j = lax.rem(b + s, q)
            total = a1[zk, a, j].astype(jnp.float32)
            for r in range(1, q):
                total = total + r_a[r - 1, zk, j].astype(jnp.float32)
            a2[zk, j] = total.astype(a2.dtype)
            if s < q:
                copy = remote(
                    a2.at[zk, j], r_b.at[s - 1, zk], b_sem, (s - 1, k), device(z, a, j)
                )
                copy.start()
                b_copies.append(copy)

    def reduce_b(k):
        zk = order[k]
        for s in range(1, q):
            b_copies[k * (q - 1) + s - 1].wait_recv()
        total = a2[zk, b].astype(jnp.float32)
        for s in range(1, q):
            total = total + r_b[s - 1, zk].astype(jnp.float32)
        if k < nz - 1:
            a3[k] = total.astype(a3.dtype)
            copy = remote(a3.at[k], r_z.at[k], z_sem, (k,), device(zk, a, b))
            copy.start()
            z_copies.append(copy)
        else:
            mine[...] = total

    for k in range(nz + 3):
        if k < nz:
            flatten(order[k])
            if k == 0:
                pl.semaphore_wait(barrier, n - 1)
            copy = remote(g.at[1 - c, order[k]], r0.at[order[k]], c_sem, (k,), partner)
            copy.start()
            c_copies.append(copy)
        if 0 <= k - 1 < nz:
            reduce_core(k - 1)
        if 0 <= k - 2 < nz:
            reduce_a(k - 2)
        if 0 <= k - 3 < nz:
            reduce_b(k - 3)
    for copy in z_copies:
        copy.wait_recv()
    total = mine[...]
    for k in range(nz - 1):
        total = total + r_z[k].astype(jnp.float32)
    mine[...] = total

    norm_src[...] = jnp.sum(total * total, axis=0, keepdims=True)
    norm_all[me] = norm_src[...]

    @pl.loop(1, n)
    def _(r):
        remote(norm_src, norm_all.at[me], n_sem, (), lax.rem(me + r, n)).start()

    others = norm_all.at[pl.ds(0, n - 1)]
    norm_copies = remote(others, others, n_sem, (), partner)
    norm_copies.wait_recv()
    norm = jnp.sqrt(jnp.sum(jnp.sum(norm_all[...], axis=0), axis=1, keepdims=True))
    clip = jnp.minimum(jnp.float32(1.0), max_norm / (norm + 1e-06))
    norm_out[...] = jnp.broadcast_to(norm, norm_out.shape)

    step, new = adamw_update(
        mine[base_p : base_p + flat_p], clip, master_p[...], moment_p[...], second_p[...]
    )
    step_p[...] = step
    new_p[...] = new
    stage[base_p : base_p + flat_p] = new
    step, new = adamw_update(mine[:flat_e], clip, master_e[...], moment_e[...], second_e[...])
    step_e[...] = step
    new_e[...] = new
    stage[:flat_e] = new
    w[c, z, a, b] = stage[:depth].astype(w.dtype)

    sent = []

    def forward(block, z_at, sems, at, target):
        copy = remote(block, block, sems, at, target)
        copy.start()
        sent.append(copy)

    def back(index, by, size):
        return lax.rem(index + size - by, size)

    own = w.at[c, z, a, b]
    for k in range(nz - 1):
        forward(own, z, gz_sem, (k,), device(order[k], a, b))

    def gather_z(t):
        z_t = back(z, t, nz)
        block = w.at[c, z_t, a, b]
        if t:
            remote(block, block, gz_sem, (t - 1,), partner).wait_recv()
        for s in range(1, q):
            forward(block, z_t, gb_sem, (s - 1, t), device(z, a, lax.rem(b + s, q)))
        for s in range(1, q):
            forward(block, z_t, ga_sem, (s - 1, t, 0), device(z, lax.rem(a + s, q), b))
        forward(block, z_t, gc_sem, (t, 0, 0), partner)

    def gather_b(t):
        z_t = back(z, t, nz)
        for kb in range(1, q):
            block = w.at[c, z_t, a, back(b, kb, q)]
            remote(block, block, gb_sem, (kb - 1, t), partner).wait_recv()
            for s in range(1, q):
                forward(block, z_t, ga_sem, (s - 1, t, kb), device(z, lax.rem(a + s, q), b))
            forward(block, z_t, gc_sem, (t, kb, 0), partner)

    def gather_a(t):
        z_t = back(z, t, nz)
        for kb in range(q):
            for ka in range(1, q):
                block = w.at[c, z_t, back(a, ka, q), back(b, kb, q)]
                remote(block, block, ga_sem, (ka - 1, t, kb), partner).wait_recv()
                forward(block, z_t, gc_sem, (t, kb, ka), partner)

    def unflatten(t):
        z_t = back(z, t, nz)
        for kb in range(q):
            for ka in range(q):
                block = w.at[1 - c, z_t, back(b, ka, q), back(a, kb, q)]
                remote(block, block, gc_sem, (t, kb, ka), partner).wait_recv()

        @pl.loop(z_t * groups, z_t * groups + groups)
        def _(p):
            top_p = pl.multiple_of(p * (group * rows), 16)
            top_e = pl.multiple_of(p * (group * rows_embed), 16)
            for i in range(group):
                core, dz, da, db = place(p * group + i)
                stage[i * depth : (i + 1) * depth] = w[core, dz, da, db].astype(jnp.float32)
            for j in range(columns):
                lanes = slice(j * LANES, (j + 1) * LANES)
                weight_p[pl.ds(top_p, group * rows), lanes] = jnp.concatenate(
                    [
                        stage[pl.ds(i * depth + base_p + j, rows, stride=columns), :]
                        for i in range(group)
                    ],
                    axis=0,
                ).astype(weight_p.dtype)
                weight_e[pl.ds(top_e, group * rows_embed), lanes] = jnp.concatenate(
                    [
                        stage[pl.ds(i * depth + j, rows_embed, stride=columns), :]
                        for i in range(group)
                    ],
                    axis=0,
                ).astype(weight_e.dtype)

    for t in range(nz + 3):
        if t < nz:
            gather_z(t)
        if 0 <= t - 1 < nz:
            gather_b(t - 1)
        if 0 <= t - 2 < nz:
            gather_a(t - 2)
        if 0 <= t - 3 < nz:
            unflatten(t - 3)

    next_e[...] = jnp.dot(
        freq_next[...], weight_e[...], preferred_element_type=jnp.float32
    ).astype(next_e.dtype)

    @pl.loop(0, weight_p.shape[1] // span)
    def _(i):
        left = pl.multiple_of(i * span, span)
        next_p[:, pl.ds(left, span)] = jnp.dot(
            attended_next[...], weight_p[:, pl.ds(left, span)], preferred_element_type=jnp.float32
        ).astype(next_p.dtype)

    for copy in c_copies + a_copies + b_copies + z_copies + sent:
        copy.wait_send()
    norm_copies.wait_send()


def block_of(width):
    return next(size for size in (384, 256, 128) if width % size == 0)


def copy_kernel(*refs):
    half = len(refs) // 2
    for source, result in zip(refs[:half], refs[half:]):
        result[...] = source[...]


def exchange(n, attended, proj_cot, freq_now, embed_cot, attended_next, freq_next, states):
    nz, ny, nx = factor(n)
    width = attended.shape[1]
    width_e = freq_now.shape[0]
    columns = width // LANES
    rows, rows_embed = width // n, width_e // n
    group = max(16 // math.gcd(rows, 16), 16 // math.gcd(rows_embed, 16))
    depth = round_up(round_up(rows_embed * columns, 8) + rows * columns, 16)
    f32, bf16 = jnp.float32, jnp.bfloat16
    q = nx
    assert nx == ny and n % (group * nz) == 0

    def dma(*sizes):
        return pltpu.SemaphoreType.DMA((2, *(max(size, 1) for size in sizes)))

    flat_p = jax.ShapeDtypeStruct((rows * columns, LANES), f32)
    flat_e = jax.ShapeDtypeStruct((rows_embed * columns, LANES), f32)
    vmem = pl.BlockSpec(memory_space=pltpu.VMEM)
    results = (
        jax.ShapeDtypeStruct(attended_next.shape, bf16),
        jax.ShapeDtypeStruct(embed_cot.shape, bf16),
        flat_p,
        flat_e,
        flat_p,
        flat_e,
        jax.ShapeDtypeStruct((1, LANES), f32),
    )
    outs = pl.pallas_call(
        functools.partial(exchange_kernel, n, rows, rows_embed),
        out_shape=results,
        in_specs=[vmem] * 12,
        out_specs=(vmem,) * 7,
        scratch_shapes=[
            pltpu.VMEM((width, width), f32),
            pltpu.VMEM((width_e, width), f32),
            pltpu.VMEM((width, width), bf16),
            pltpu.VMEM((width_e, width), bf16),
            pltpu.VMEM((group * depth, LANES), f32),
            pltpu.VMEM((depth, LANES), f32),
            pltpu.VMEM((2, nz, q, q, depth, LANES), bf16),
            pltpu.VMEM((nz, q, q, depth, LANES), bf16),
            pltpu.VMEM((nz, q, q, depth, LANES), bf16),
            pltpu.VMEM((q - 1, nz, q, depth, LANES), bf16),
            pltpu.VMEM((nz, q, depth, LANES), bf16),
            pltpu.VMEM((q - 1, nz, depth, LANES), bf16),
            pltpu.VMEM((nz - 1, depth, LANES), bf16),
            pltpu.VMEM((nz - 1, depth, LANES), bf16),
            pltpu.VMEM((1, LANES), f32),
            pltpu.VMEM((n, 1, LANES), f32),
            pltpu.VMEM((2, nz, q, q, depth, LANES), bf16),
            dma(nz),
            dma(q - 1, nz),
            dma(q - 1, nz),
            dma(nz - 1),
            dma(),
            dma(nz - 1),
            dma(q - 1, nz),
            dma(q - 1, nz, q),
            dma(nz, q, q),
        ],
        compiler_params=pltpu.CompilerParams(
            collective_id=0, has_side_effects=True, vmem_limit_bytes=VMEM_LIMIT
        ),
    )(
        attended,
        proj_cot,
        freq_now,
        embed_cot,
        attended_next,
        freq_next,
        *(state.reshape(-1, LANES) for state in states),
    )
    return pl.pallas_call(
        copy_kernel,
        out_shape=results,
        in_specs=[vmem] * 7,
        out_specs=(vmem,) * 7,
        compiler_params=pltpu.CompilerParams(vmem_limit_bytes=VMEM_LIMIT),
    )(*outs)


def per_device(
    attended,
    proj_cot,
    timesteps,
    embed_cot,
    master_proj,
    moment_proj,
    second_proj,
    master_embed,
    moment_embed,
    squared_moment_layer,
    attended_next,
    timesteps_next,
):
    width = attended.shape[1]
    freq_width = master_embed.shape[0] * lax.axis_size("dp") // width
    n = lax.axis_size("dp")
    freq_now = freq_embed(timesteps, freq_width).astype(jnp.float32).T
    freq_next = freq_embed(timesteps_next, freq_width)
    states = (
        master_proj,
        moment_proj,
        second_proj,
        master_embed,
        moment_embed,
        squared_moment_layer,
    )
    next_proj, next_embed, step_p, step_e, new_p, new_e, norm = exchange(
        n, attended, proj_cot, freq_now, embed_cot, attended_next, freq_next, states
    )
    return (
        next_proj,
        next_embed,
        step_p.reshape(-1),
        step_e.reshape(-1),
        new_p.reshape(-1),
        new_e.reshape(-1),
        norm[0, 0],
    )


def solution(mesh):
    in_specs = (
        P("dp", None),
        P("dp", None),
        P("dp"),
        P("dp", None),
        P("dp"),
        P("dp"),
        P("dp"),
        P("dp"),
        P("dp"),
        P("dp"),
        P("dp", None),
        P("dp"),
    )
    out_specs = (P("dp", None), P("dp", None), P("dp"), P("dp"), P("dp"), P("dp"), P())
    return jax.shard_map(
        per_device, mesh=mesh, in_specs=in_specs, out_specs=out_specs, check_vma=False
    )
```

```python
import functools
import math

import jax
import jax.numpy as jnp
from jax import lax
from jax.experimental import pallas as pl
from jax.experimental.pallas import tpu as pltpu
from jax.sharding import PartitionSpec as P

beta_one = 0.9
beta_two = 0.999
step_count = 1000.0
learn_rate = 0.0001
shrink_factor = 0.01
epsilon = 1e-08
max_norm = 1.0


def freq_embed(moments, width):
    half_width = width // 2
    ladder = jnp.arange(half_width, dtype=jnp.float32)
    freqs = jnp.exp(-math.log(10000.0) * ladder / half_width)
    phase_values = (moments * 1000.0)[:, None] * freqs[None, :]
    return jnp.concatenate([jnp.cos(phase_values), jnp.sin(phase_values)], axis=1).astype(
        jnp.bfloat16
    )


def adamw_update(gradient, clip, master, moment, second):
    scaled = clip * gradient
    first_new = beta_one * moment + (1.0 - beta_one) * scaled
    second_new = beta_two * second + (1.0 - beta_two) * scaled * scaled
    first_hat = first_new / (1.0 - beta_one**step_count)
    second_hat = second_new / (1.0 - beta_two**step_count)
    direction = first_hat / (jnp.sqrt(second_hat) + epsilon)
    freshened_values = master - learn_rate * (direction + shrink_factor * master)
    return (direction, freshened_values)


LANES = 128
VMEM_LIMIT = 62 * 2**20
MESH = pl.DeviceIdType.MESH


def round_up(value, step):
    return -(-value // step) * step


def factor(n):
    bits = (n // 2).bit_length() - 1
    z_bits = -(-bits // 3)
    y_bits = -(-(bits - z_bits) // 2)
    return 2**z_bits, 2**y_bits, 2 ** (bits - z_bits - y_bits)


def exchange_kernel(
    n,
    rows,
    rows_embed,
    attended,
    proj_cot,
    freq_now,
    embed_cot,
    attended_next,
    freq_next,
    master_p,
    moment_p,
    second_p,
    master_e,
    moment_e,
    second_e,
    next_p,
    next_e,
    step_p,
    step_e,
    new_p,
    new_e,
    norm_out,
    grad_p,
    grad_e,
    weight_p,
    weight_e,
    stage,
    mine,
    g,
    r0,
    a1,
    r_a,
    a2,
    r_b,
    a3,
    r_z,
    norm_src,
    norm_all,
    w,
    c_sem,
    a_sem,
    b_sem,
    z_sem,
    n_sem,
    gz_sem,
    gb_sem,
    ga_sem,
    gc_sem,
):
    nz, ny, nx = factor(n)
    q = nx
    columns = grad_p.shape[1] // LANES
    flat_e = rows_embed * columns
    flat_p = rows * columns
    base_p = round_up(flat_e, 8)
    depth = g.shape[-2]
    group = stage.shape[0] // depth

    me = lax.axis_index("dp")
    c = lax.rem(me, 2)
    x = lax.rem(me // 2, nx)
    y = lax.rem(me // (2 * nx), ny)
    z = me // (2 * nx * ny)
    first = c == 0
    a, b = jnp.where(first, x, y), jnp.where(first, y, x)
    stride_a, stride_b = jnp.where(first, 2, 2 * nx), jnp.where(first, 2 * nx, 2)

    def device(z_at, a_at, b_at):
        return z_at * (2 * nx * ny) + a_at * stride_a + b_at * stride_b + c

    partner = me + 1 - 2 * c

    def place(d):
        core = lax.rem(d, 2)
        dx = lax.rem(d // 2, nx)
        dy = lax.rem(d // (2 * nx), ny)
        return (
            core,
            d // (2 * nx * ny),
            jnp.where(core == 0, dx, dy),
            jnp.where(core == 0, dy, dx),
        )

    def remote(src, dst, sems, at, target):
        return pltpu.make_async_remote_copy(
            src_ref=src,
            dst_ref=dst,
            send_sem=sems.at[(0, *at)],
            recv_sem=sems.at[(1, *at)],
            device_id=(target,),
            device_id_type=MESH,
        )

    barrier = pltpu.get_barrier_semaphore()

    @pl.loop(1, n)
    def _(r):
        pl.semaphore_signal(
            barrier, inc=1, device_id=(lax.rem(me + r, n),), device_id_type=MESH
        )

    span = block_of(attended.shape[1])

    @pl.loop(0, attended.shape[1] // span)
    def _(i):
        top = pl.multiple_of(i * span, span)
        grad_p[pl.ds(top, span), :] = lax.dot_general(
            attended[:, pl.ds(top, span)],
            proj_cot[...],
            (((0,), (0,)), ((), ())),
            preferred_element_type=jnp.float32,
        )

    grad_e[...] = lax.dot_general(
        freq_now[...],
        embed_cot[...],
        (((0,), (0,)), ((), ())),
        preferred_element_type=jnp.float32,
    )

    stage[...] = jnp.zeros_like(stage)
    order = [lax.rem(z + 1 + k, nz) for k in range(nz)]
    groups = n // group // nz
    c_copies, a_copies, b_copies, z_copies = [], [], [], []

    def flatten(zk):
        @pl.loop(zk * groups, zk * groups + groups)
        def _(p):
            top_p = pl.multiple_of(p * (group * rows), 16)
            top_e = pl.multiple_of(p * (group * rows_embed), 16)
            for j in range(columns):
                lanes = slice(j * LANES, (j + 1) * LANES)
                values_p = grad_p[pl.ds(top_p, group * rows), lanes]
                values_e = grad_e[pl.ds(top_e, group * rows_embed), lanes]
                for i in range(group):
                    stage[pl.ds(i * depth + base_p + j, rows, stride=columns), :] = values_p[
                        i * rows : (i + 1) * rows
                    ]
                    stage[pl.ds(i * depth + j, rows_embed, stride=columns), :] = values_e[
                        i * rows_embed : (i + 1) * rows_embed
                    ]
            for i in range(group):
                core, dz, da, db = place(p * group + i)
                g[core, dz, da, db] = stage[i * depth : (i + 1) * depth].astype(g.dtype)

    def reduce_core(k):
        zk = order[k]
        c_copies[k].wait_recv()
        for s in range(1, q + 1):
            i = lax.rem(a + s, q)
            for j in range(q):
                a1[zk, i, j] = (
                    g[c, zk, i, j].astype(jnp.float32) + r0[zk, i, j].astype(jnp.float32)
                ).astype(a1.dtype)
            if s < q:
                copy = remote(
                    a1.at[zk, i], r_a.at[s - 1, zk], a_sem, (s - 1, k), device(z, i, b)
                )
                copy.start()
                a_copies.append(copy)

    def reduce_a(k):
        zk = order[k]
        for s in range(1, q):
            a_copies[k * (q - 1) + s - 1].wait_recv()
        for s in range(1, q + 1):
            j = lax.rem(b + s, q)
            total = a1[zk, a, j].astype(jnp.float32)
            for r in range(1, q):
                total = total + r_a[r - 1, zk, j].astype(jnp.float32)
            a2[zk, j] = total.astype(a2.dtype)
            if s < q:
                copy = remote(
                    a2.at[zk, j], r_b.at[s - 1, zk], b_sem, (s - 1, k), device(z, a, j)
                )
                copy.start()
                b_copies.append(copy)

    def reduce_b(k):
        zk = order[k]
        for s in range(1, q):
            b_copies[k * (q - 1) + s - 1].wait_recv()
        total = a2[zk, b].astype(jnp.float32)
        for s in range(1, q):
            total = total + r_b[s - 1, zk].astype(jnp.float32)
        if k < nz - 1:
            a3[k] = total.astype(a3.dtype)
            copy = remote(a3.at[k], r_z.at[k], z_sem, (k,), device(zk, a, b))
            copy.start()
            z_copies.append(copy)
        else:
            mine[...] = total

    for k in range(nz + 3):
        if k < nz:
            flatten(order[k])
            if k == 0:
                pl.semaphore_wait(barrier, n - 1)
            copy = remote(g.at[1 - c, order[k]], r0.at[order[k]], c_sem, (k,), partner)
            copy.start()
            c_copies.append(copy)
        if 0 <= k - 1 < nz:
            reduce_core(k - 1)
        if 0 <= k - 2 < nz:
            reduce_a(k - 2)
        if 0 <= k - 3 < nz:
            reduce_b(k - 3)
    for copy in z_copies:
        copy.wait_recv()
    total = mine[...]
    for k in range(nz - 1):
        total = total + r_z[k].astype(jnp.float32)
    mine[...] = total

    norm_src[...] = jnp.sum(total * total, axis=0, keepdims=True)
    norm_all[me] = norm_src[...]

    @pl.loop(1, n)
    def _(r):
        remote(norm_src, norm_all.at[me], n_sem, (), lax.rem(me + r, n)).start()

    others = norm_all.at[pl.ds(0, n - 1)]
    norm_copies = remote(others, others, n_sem, (), partner)
    norm_copies.wait_recv()
    norm = jnp.sqrt(jnp.sum(jnp.sum(norm_all[...], axis=0), axis=1, keepdims=True))
    clip = jnp.minimum(jnp.float32(1.0), max_norm / (norm + 1e-06))
    norm_out[...] = jnp.broadcast_to(norm, norm_out.shape)

    step, new = adamw_update(
        mine[base_p : base_p + flat_p], clip, master_p[...], moment_p[...], second_p[...]
    )
    step_p[...] = step
    new_p[...] = new
    stage[base_p : base_p + flat_p] = new
    step, new = adamw_update(mine[:flat_e], clip, master_e[...], moment_e[...], second_e[...])
    step_e[...] = step
    new_e[...] = new
    stage[:flat_e] = new
    w[c, z, a, b] = stage[:depth].astype(w.dtype)

    sent = []

    def forward(block, z_at, sems, at, target):
        copy = remote(block, block, sems, at, target)
        copy.start()
        sent.append(copy)

    def back(index, by, size):
        return lax.rem(index + size - by, size)

    own = w.at[c, z, a, b]
    for k in range(nz - 1):
        forward(own, z, gz_sem, (k,), device(order[k], a, b))

    def gather_z(t):
        z_t = back(z, t, nz)
        block = w.at[c, z_t, a, b]
        if t:
            remote(block, block, gz_sem, (t - 1,), partner).wait_recv()
        for s in range(1, q):
            forward(block, z_t, gb_sem, (s - 1, t), device(z, a, lax.rem(b + s, q)))
        for s in range(1, q):
            forward(block, z_t, ga_sem, (s - 1, t, 0), device(z, lax.rem(a + s, q), b))
        forward(block, z_t, gc_sem, (t, 0, 0), partner)

    def gather_b(t):
        z_t = back(z, t, nz)
        for kb in range(1, q):
            block = w.at[c, z_t, a, back(b, kb, q)]
            remote(block, block, gb_sem, (kb - 1, t), partner).wait_recv()
            for s in range(1, q):
                forward(block, z_t, ga_sem, (s - 1, t, kb), device(z, lax.rem(a + s, q), b))
            forward(block, z_t, gc_sem, (t, kb, 0), partner)

    def gather_a(t):
        z_t = back(z, t, nz)
        for kb in range(q):
            for ka in range(1, q):
                block = w.at[c, z_t, back(a, ka, q), back(b, kb, q)]
                remote(block, block, ga_sem, (ka - 1, t, kb), partner).wait_recv()
                forward(block, z_t, gc_sem, (t, kb, ka), partner)

    def unflatten(t):
        z_t = back(z, t, nz)
        for kb in range(q):
            for ka in range(q):
                block = w.at[1 - c, z_t, back(b, ka, q), back(a, kb, q)]
                remote(block, block, gc_sem, (t, kb, ka), partner).wait_recv()

        @pl.loop(z_t * groups, z_t * groups + groups)
        def _(p):
            top_p = pl.multiple_of(p * (group * rows), 16)
            top_e = pl.multiple_of(p * (group * rows_embed), 16)
            for i in range(group):
                core, dz, da, db = place(p * group + i)
                stage[i * depth : (i + 1) * depth] = w[core, dz, da, db].astype(jnp.float32)
            for j in range(columns):
                lanes = slice(j * LANES, (j + 1) * LANES)
                weight_p[pl.ds(top_p, group * rows), lanes] = jnp.concatenate(
                    [
                        stage[pl.ds(i * depth + base_p + j, rows, stride=columns), :]
                        for i in range(group)
                    ],
                    axis=0,
                ).astype(weight_p.dtype)
                weight_e[pl.ds(top_e, group * rows_embed), lanes] = jnp.concatenate(
                    [
                        stage[pl.ds(i * depth + j, rows_embed, stride=columns), :]
                        for i in range(group)
                    ],
                    axis=0,
                ).astype(weight_e.dtype)

    for t in range(nz + 3):
        if t < nz:
            gather_z(t)
        if 0 <= t - 1 < nz:
            gather_b(t - 1)
        if 0 <= t - 2 < nz:
            gather_a(t - 2)
        if 0 <= t - 3 < nz:
            unflatten(t - 3)

    next_e[...] = jnp.dot(
        freq_next[...], weight_e[...], preferred_element_type=jnp.float32
    ).astype(next_e.dtype)

    @pl.loop(0, weight_p.shape[1] // span)
    def _(i):
        left = pl.multiple_of(i * span, span)
        next_p[:, pl.ds(left, span)] = jnp.dot(
            attended_next[...], weight_p[:, pl.ds(left, span)], preferred_element_type=jnp.float32
        ).astype(next_p.dtype)

    for copy in c_copies + a_copies + b_copies + z_copies + sent:
        copy.wait_send()
    norm_copies.wait_send()


def block_of(width):
    return next(size for size in (384, 256, 128) if width % size == 0)


def copy_kernel(*refs):
    half = len(refs) // 2
    for source, result in zip(refs[:half], refs[half:]):
        result[...] = source[...]


def exchange(n, attended, proj_cot, freq_now, embed_cot, attended_next, freq_next, states):
    nz, ny, nx = factor(n)
    width = attended.shape[1]
    width_e = freq_now.shape[1]
    columns = width // LANES
    rows, rows_embed = width // n, width_e // n
    group = max(16 // math.gcd(rows, 16), 16 // math.gcd(rows_embed, 16))
    depth = round_up(round_up(rows_embed * columns, 8) + rows * columns, 16)
    f32, bf16 = jnp.float32, jnp.bfloat16
    q = nx
    assert nx == ny and n % (group * nz) == 0

    def dma(*sizes):
        return pltpu.SemaphoreType.DMA((2, *(max(size, 1) for size in sizes)))

    flat_p = jax.ShapeDtypeStruct((rows * columns, LANES), f32)
    flat_e = jax.ShapeDtypeStruct((rows_embed * columns, LANES), f32)
    vmem = pl.BlockSpec(memory_space=pltpu.VMEM)
    results = (
        jax.ShapeDtypeStruct(attended_next.shape, bf16),
        jax.ShapeDtypeStruct(embed_cot.shape, bf16),
        flat_p,
        flat_e,
        flat_p,
        flat_e,
        jax.ShapeDtypeStruct((1, LANES), f32),
    )
    outs = pl.pallas_call(
        functools.partial(exchange_kernel, n, rows, rows_embed),
        out_shape=results,
        in_specs=[vmem] * 12,
        out_specs=(vmem,) * 7,
        scratch_shapes=[
            pltpu.VMEM((width, width), f32),
            pltpu.VMEM((width_e, width), f32),
            pltpu.VMEM((width, width), bf16),
            pltpu.VMEM((width_e, width), bf16),
            pltpu.VMEM((group * depth, LANES), f32),
            pltpu.VMEM((depth, LANES), f32),
            pltpu.VMEM((2, nz, q, q, depth, LANES), bf16),
            pltpu.VMEM((nz, q, q, depth, LANES), bf16),
            pltpu.VMEM((nz, q, q, depth, LANES), bf16),
            pltpu.VMEM((q - 1, nz, q, depth, LANES), bf16),
            pltpu.VMEM((nz, q, depth, LANES), bf16),
            pltpu.VMEM((q - 1, nz, depth, LANES), bf16),
            pltpu.VMEM((nz - 1, depth, LANES), bf16),
            pltpu.VMEM((nz - 1, depth, LANES), bf16),
            pltpu.VMEM((1, LANES), f32),
            pltpu.VMEM((n, 1, LANES), f32),
            pltpu.VMEM((2, nz, q, q, depth, LANES), bf16),
            dma(nz),
            dma(q - 1, nz),
            dma(q - 1, nz),
            dma(nz - 1),
            dma(),
            dma(nz - 1),
            dma(q - 1, nz),
            dma(q - 1, nz, q),
            dma(nz, q, q),
        ],
        compiler_params=pltpu.CompilerParams(
            collective_id=0, has_side_effects=True, vmem_limit_bytes=VMEM_LIMIT
        ),
    )(
        attended,
        proj_cot,
        freq_now,
        embed_cot,
        attended_next,
        freq_next,
        *(state.reshape(-1, LANES) for state in states),
    )
    return pl.pallas_call(
        copy_kernel,
        out_shape=results,
        in_specs=[vmem] * 7,
        out_specs=(vmem,) * 7,
        compiler_params=pltpu.CompilerParams(vmem_limit_bytes=VMEM_LIMIT),
    )(*outs)


def per_device(
    attended,
    proj_cot,
    timesteps,
    embed_cot,
    master_proj,
    moment_proj,
    second_proj,
    master_embed,
    moment_embed,
    squared_moment_layer,
    attended_next,
    timesteps_next,
):
    width = attended.shape[1]
    freq_width = master_embed.shape[0] * lax.axis_size("dp") // width
    n = lax.axis_size("dp")
    freq_now = freq_embed(timesteps, freq_width)
    freq_next = freq_embed(timesteps_next, freq_width)
    states = (
        master_proj,
        moment_proj,
        second_proj,
        master_embed,
        moment_embed,
        squared_moment_layer,
    )
    next_proj, next_embed, step_p, step_e, new_p, new_e, norm = exchange(
        n, attended, proj_cot, freq_now, embed_cot, attended_next, freq_next, states
    )
    return (
        next_proj,
        next_embed,
        step_p.reshape(-1),
        step_e.reshape(-1),
        new_p.reshape(-1),
        new_e.reshape(-1),
        norm[0, 0],
    )


def solution(mesh):
    in_specs = (
        P("dp", None),
        P("dp", None),
        P("dp"),
        P("dp", None),
        P("dp"),
        P("dp"),
        P("dp"),
        P("dp"),
        P("dp"),
        P("dp"),
        P("dp", None),
        P("dp"),
    )
    out_specs = (P("dp", None), P("dp", None), P("dp"), P("dp"), P("dp"), P("dp"), P())
    return jax.shard_map(
        per_device, mesh=mesh, in_specs=in_specs, out_specs=out_specs, check_vma=False
    )
```
